32 devices in a mesh: expert: 8 (over y, x, core), row: 4 (over z).
Axes of the slice: x: 2, y: 2, z: 4, core: 2. Of those that a mesh axis runs over, the one named last changes fastest.
Arguments:
- weights: bfloat16 [8, 7168, 2048], P('expert', 'row'), may hold values from -6 to 6
- left_bits: int32 [8, 7168], P('expert', 'row'), may hold values from 0 to 1
- right_bits: int32 [8, 2048], P('expert'), may hold values from 0 to 1
- groups: int32 [8, 2048], P('expert'), may hold values from 0 to 15, never falling along the last dimension, each value on 1 to 256 neighbouring positions
Outputs:
- scaled: bfloat16 [8, 7168, 2048], P('expert', 'row')
- block_error: float32 [8, 7168, 256], P('expert', 'row')
- scales: float32 [8, 16], P('expert')
- expert_error: float32 [8], P('expert')
- total_error: float32 [], replicated
The draws below stay inside these ranges and needn't reach their ends.
Inputs may be any that keep to these rules, and one draw needn't show every extreme that they name: Along each expert's 2048 columns the group number never falls; each of the 16 groups holds 1 to 256 columns.
All inputs are finite; a program needn't handle non-finite values.
Results may differ from the reference program's by a relative error of at most 0.0091.
Values may be sent and summed in bfloat16 or wider, within the bound.
A program may use at most 192 MiB of HBM per device.

```python
import math
import jax
import jax.numpy as jnp
import numpy as np
from jax import lax

D = 7168
FF = 2048
HB = 128
OUTER = 16
GROUPS = 16
BLOCKS = 56
GROUP_MOST = 256
EXPERTS = 8


def draw_weights(key, part):
    scale_key = jax.random.fold_in(key, 11)
    entry_key = jax.random.fold_in(key, 12)
    magnitude = jnp.exp(jax.random.uniform(scale_key, (EXPERTS, 1, 1), jnp.float32, math.log(0.02), math.log(1.0)))
    entries = jnp.clip(jax.random.normal(entry_key, (EXPERTS, D, FF), jnp.float32), -6.0, 6.0)
    return jnp.clip(entries * magnitude, -6.0, 6.0).astype(jnp.bfloat16)


def place_ends(result, stream_key, low, high):
    longest = result.shape.index(max(result.shape))
    spots = []
    for shift in (0, 1):
        where = [jax.random.randint(jax.random.fold_in(stream_key, axis), (), 0, length) for axis, length in enumerate(result.shape)]
        where[longest] = (where[longest] + shift) % result.shape[longest]
        spots.append(tuple(where))
    return result.at[spots[0]].set(low).at[spots[1]].set(high)


def profile(number_of, total, most, slope):
    loads = [(1 << 20) // math.isqrt(grade ** slope) + 1 for grade in range(2, number_of + 1)]
    spare, holding = total - most - (number_of - 1), [1] * (number_of - 1)
    while spare > 0:
        free = [i for i in range(number_of - 1) if holding[i] < most]
        whole, left = sum([loads[i] for i in free]), spare
        for i in free:
            more = min(most - holding[i], max(1, left * loads[i] // whole), spare)
            holding[i] = holding[i] + more
            spare = spare - more
    return np.array([most] + holding)


def ragged(key, amount, total, bound, skew):
    if amount == 2:
        one = jax.random.randint(key, (), max(1, total - bound), min(bound, total - 1) + 1)
        return jnp.stack([one, total - one])
    lengths = jnp.asarray(profile(amount, total, bound, skew), jnp.int32)
    couples = (amount - 1) // 2
    donor, receiver = lengths[1:1 + 2 * couples:2], lengths[2:2 + 2 * couples:2]
    room = jnp.minimum(donor - 1, bound - receiver)
    passed = jax.random.randint(jax.random.fold_in(key, 1), (couples,), 0, 1 << 20) % (room + 1)
    lengths = lengths.at[1:1 + 2 * couples:2].set(donor - passed).at[2:2 + 2 * couples:2].set(receiver + passed)
    return lengths[jax.random.permutation(jax.random.fold_in(key, 2), amount)]


def setup_inputs(seed: int = 0) -> dict:
    streams_of = jax.random.split(jax.random.key(seed), 5)
    return {
        "weights": draw_weights(jax.random.fold_in(streams_of[4], 71), 0),
        "left_bits": place_ends(jax.random.randint(streams_of[1], (EXPERTS, D), 0, 2), jax.random.fold_in(streams_of[1], 1), 0, 1).astype(jnp.int32),
        "right_bits": place_ends(jax.random.randint(streams_of[2], (EXPERTS, FF), 0, 2), jax.random.fold_in(streams_of[2], 1), 0, 1).astype(jnp.int32),
        "groups": jax.vmap(lambda own: jnp.searchsorted(jnp.cumsum(ragged(own, GROUPS, FF, GROUP_MOST, 1)), jnp.arange(FF), side="right"))(jax.random.split(streams_of[3], EXPERTS)).reshape((EXPERTS, FF)).astype(jnp.int32),
    }


def sylvester(order):
    row_index = jnp.arange(order, dtype=jnp.int32)[:, None]
    col_index = jnp.arange(order, dtype=jnp.int32)[None, :]
    common = jnp.bitwise_and(row_index, col_index)
    parity = jnp.zeros((order, order), jnp.int32)
    for bit_pos in range(order.bit_length() - 1):
        parity = parity + jnp.bitwise_and(jnp.right_shift(common, bit_pos), 1)
    return (1 - 2 * jnp.bitwise_and(parity, 1)).astype(jnp.float32)

def cosine_block(order):
    first = jnp.arange(order, dtype=jnp.float32)[:, None]
    second = jnp.arange(order, dtype=jnp.float32)[None, :]
    table = math.sqrt(2.0 / order) * jnp.cos(math.pi * (2.0 * second + 1.0) * first / (2.0 * order))
    return jnp.where(first == 0.0, table * math.sqrt(0.5), table)

def coset_error(values):
    nearest = jnp.floor(values + 0.5)
    offset = values - nearest
    squares = lax.optimization_barrier(jnp.sum(offset * offset, axis=-1))
    largest = lax.optimization_barrier(jnp.max(jnp.abs(offset), axis=-1))
    parity = jnp.mod(lax.optimization_barrier(jnp.sum(nearest, axis=-1)), 2.0)
    return jnp.where(parity > 0.5, squares + 1.0 - 2.0 * largest, squares)

def lattice_error(values):
    octets = values.reshape(values.shape[:-1] + (values.shape[-1] // 8, 8))
    return jnp.minimum(coset_error(octets), coset_error(octets - 0.5))

def reference(weights, left_bits, right_bits, groups):
    column_hadamard = sylvester(FF // OUTER)
    outer_hadamard = sylvester(OUTER)
    row_hadamard = sylvester(HB)
    block_matrix = cosine_block(BLOCKS).astype(jnp.bfloat16).astype(jnp.float32)
    group_ids = jnp.arange(GROUPS, dtype=jnp.int32)
    row_weight = (1.0 + 4.0 * (jnp.arange(D, dtype=jnp.float32) + 0.5) / D) / 3.0
    high = lax.Precision.HIGHEST

    def one_expert(operands):
        weight, left, right, group = operands
        left_sign = (2 * left - 1).astype(jnp.float32)
        right_sign = (2 * right - 1).astype(jnp.float32)
        signed = (weight.astype(jnp.float32) * left_sign[:, None] * right_sign[None, :]).astype(jnp.bfloat16)
        shaped = signed.astype(jnp.float32).reshape(D, OUTER, FF // OUTER)
        inner = jnp.einsum('dpq,qs->dps', shaped, column_hadamard, precision=high)
        outer = jnp.einsum('dps,pt->dts', inner, outer_hadamard, precision=high)
        columns = (outer.reshape(D, FF) / math.sqrt(FF)).astype(jnp.bfloat16)
        blocked = columns.astype(jnp.float32).reshape(BLOCKS, HB, FF)
        mixed_rows = jnp.einsum('ij,jbf->ibf', block_matrix, blocked, precision=high)
        rotated = jnp.einsum('ibf,bk->ikf', mixed_rows, row_hadamard, precision=high) / math.sqrt(HB)
        rotated = rotated.reshape(D, FF)
        column_peak = lax.optimization_barrier(jnp.max(jnp.abs(rotated), axis=0))
        in_group = group[None, :] == group_ids[:, None]
        group_peak = jnp.maximum(lax.optimization_barrier(jnp.max(jnp.where(in_group, column_peak[None, :], 0.0), axis=1)), 1.0)
        column_scale = lax.optimization_barrier(jnp.sum(jnp.where(in_group, (2.0 / group_peak)[:, None], 0.0), axis=0))
        values = rotated * column_scale[None, :]
        block_errors = lattice_error(values)
        mean_error = jnp.sum(block_errors * row_weight[:, None]) / (D * FF // 8)
        return (values.astype(jnp.bfloat16), block_errors, group_peak / 2.0, mean_error)
    scaled, block_error, scales, expert_error = lax.map(one_expert, (weights, left_bits, right_bits, groups))
    total_error = jnp.mean(expert_error)
    return (scaled, block_error, scales, expert_error, total_error)
```

```python
import functools
import math

import jax
import jax.numpy as jnp
from jax import lax
from jax.experimental import pallas as pl
from jax.experimental.pallas import tpu as pltpu
from jax.sharding import PartitionSpec as P

HB = 128
SUB = 16
FOLD = HB // SUB
OCT = 8
LANES = 128
GROUPS = 16
BLOCKS = 56
MESH = pl.DeviceIdType.MESH


def signs(common, bits):
    parity = common & 1
    for bit_pos in range(1, bits):
        parity = parity + ((common >> bit_pos) & 1)
    return (1 - 2 * (parity & 1)).astype(jnp.float32)


def cosine_block(order):
    first = jnp.arange(order, dtype=jnp.float32)[:, None]
    second = jnp.arange(order, dtype=jnp.float32)[None, :]
    table = math.sqrt(2.0 / order) * jnp.cos(math.pi * (2.0 * second + 1.0) * first / (2.0 * order))
    return jnp.where(first == 0.0, table * math.sqrt(0.5), table)


def column_matrix(right_bits, peers, half, scale):
    slabs = OCT // peers
    shape = (2, peers, half, slabs, LANES)
    row = lax.broadcasted_iota(jnp.int32, shape, 2)
    slab = lax.broadcasted_iota(jnp.int32, shape, 1) * slabs + lax.broadcasted_iota(jnp.int32, shape, 3)
    col = lax.broadcasted_iota(jnp.int32, shape, 4) * OCT + slab
    sign = (2 * right_bits - 1).astype(jnp.float32).reshape(2, 1, half, 1, 1)
    full = signs(row & col, half.bit_length() - 1) * sign * scale
    return full.astype(jnp.bfloat16).reshape(2, peers, half, slabs * LANES)


def row_matrix():
    cosine = cosine_block(BLOCKS).astype(jnp.bfloat16).astype(jnp.float32)
    index = jnp.arange(SUB, dtype=jnp.int32)
    small = signs(index[:, None] & index[None, :], SUB.bit_length() - 1)
    size = BLOCKS * SUB
    full = cosine[:, None, :, None] * small[None, :, None, :]
    return full.reshape(size, size).astype(jnp.bfloat16)


def order_matrix(half):
    source = lax.broadcasted_iota(jnp.int32, (half, half), 0)
    target = lax.broadcasted_iota(jnp.int32, (half, half), 1)
    wanted = (source % LANES) * OCT + source // LANES
    return (wanted == target).astype(jnp.bfloat16)


def fold_rows(parts):
    step = 1
    while step < len(parts):
        mixed = list(parts)
        for k in range(len(parts)):
            if not k & step:
                mixed[k] = parts[k] + parts[k + step]
                mixed[k + step] = parts[k] - parts[k + step]
        parts, step = mixed, 2 * step
    return parts


def kernel(
    peers, x_ref, left_ref, group_ref, h_ref, m_ref, p_ref,
    scaled_ref, error_ref, scale_ref, sum_ref,
    out1, in1, out2, in2, peaks, turned, scaled_stage, error_stage,
    send1, recv1, send2, recv2, send3, recv3, store_sem,
):
    blocks, _, width = x_ref.shape
    half = width // 2
    lanes = h_ref.shape[3]
    slabs = lanes // LANES
    rows = blocks * SUB
    me = lax.axis_index("row")
    far_first = sorted(range(1, peers), key=lambda d: (abs(d - peers // 2), d))
    others = [lax.rem(me + d, peers) for d in far_first]

    def remote(src, dst, send_sem, recv_sem, peer):
        return pltpu.make_async_remote_copy(
            src_ref=src, dst_ref=dst, send_sem=send_sem, recv_sem=recv_sem,
            device_id={"row": peer}, device_id_type=MESH,
        )

    def copy1(s, peer, land):
        return remote(out1.at[s, peer], in1.at[s, land], send1.at[s, peer], recv1.at[s, land], peer)

    def copy2(s, k, peer, land):
        return remote(
            out2.at[s, k, peer], in2.at[s, k, land], send2.at[s, k, peer], recv2.at[s, k, land], peer
        )

    def copy3(peer, land):
        return remote(peaks.at[me], peaks.at[land], send3.at[peer], recv3.at[land], peer)

    barrier = pltpu.get_barrier_semaphore()
    for peer in others:
        pl.semaphore_signal(barrier, inc=1, device_id={"row": peer}, device_id_type=MESH)
    pl.semaphore_wait(barrier, peers - 1)

    def column_side(peer, dst, place):
        def step(j, _):
            low = jnp.dot(x_ref[j, :, :half], h_ref[0, peer], preferred_element_type=jnp.float32)
            high = jnp.dot(x_ref[j, :, half:], h_ref[1, peer], preferred_element_type=jnp.float32)
            left = left_ref[j]
            for s, both in ((0, low + high), (1, low - high)):
                both = both * left
                parts = fold_rows([both[k * SUB:(k + 1) * SUB] for k in range(FOLD)])
                for k in range(FOLD):
                    dst[s, place, k, pl.ds(pl.multiple_of(j * SUB, SUB), SUB), :] = parts[k].astype(jnp.bfloat16)
            return 0

        lax.fori_loop(0, blocks, step, 0)

    for peer in others:
        column_side(peer, out1, peer)
        copy1(0, peer, me).start()
    for peer in others:
        copy1(1, peer, me).start()
    column_side(me, in1, me)

    def row_side(s, send):
        for peer in others:
            copy1(s, peer, peer).wait_recv()

        def step(k, peak):
            z = in1[s, :, k].reshape(peers * rows, lanes)
            r = jnp.dot(m_ref[...], z, preferred_element_type=jnp.float32)
            out2[s, k] = r.astype(jnp.bfloat16).reshape(peers, rows, lanes)
            if send:
                for peer in others:
                    copy2(s, k, peer, me).start()
            return jnp.maximum(peak, jnp.max(jnp.abs(r).reshape(-1, 8, lanes), axis=0))

        peak = lax.fori_loop(0, FOLD, step, jnp.zeros((8, lanes), jnp.float32))
        peaks[me, s] = jnp.broadcast_to(jnp.max(peak, axis=0, keepdims=True), (8, lanes))

    row_side(0, True)
    row_side(1, False)
    for peer in others:
        copy3(peer, me).start()

    def send_second(k, _):
        for peer in others:
            copy2(1, k, peer, me).start()
        return 0

    lax.fori_loop(0, FOLD, send_second, 0)

    def keep_own(k, _):
        for s in range(2):
            in2[s, k, me] = out2[s, k, me]
        return 0

    lax.fori_loop(0, FOLD, keep_own, 0)

    for peer in others:
        copy3(peer, peer).wait_recv()
    column_peak = jnp.concatenate([peaks[q, s, 0:1, :] for s in range(2) for q in range(peers)], axis=1)
    group = group_ref[...]
    column_scale = jnp.zeros_like(column_peak)
    group_scale = jnp.zeros((8, LANES), jnp.float32)
    lane = lax.broadcasted_iota(jnp.int32, (8, LANES), 1)
    for g in range(GROUPS):
        inside = group == g
        peak = jnp.maximum(jnp.max(jnp.where(inside, column_peak, 0.0), axis=1, keepdims=True), 1.0)
        column_scale = jnp.where(inside, 2.0 / peak, column_scale)
        group_scale = jnp.where(lane == g, peak * 0.5, group_scale)
    scale_ref[...] = group_scale
    sum_ref[...] = jnp.zeros_like(sum_ref)

    total_rows = peers * blocks * HB

    def stores(s, k, slot):
        return (
            pltpu.make_async_copy(
                scaled_stage.at[slot], scaled_ref.at[:, k, :, pl.ds(s * half, half)], store_sem.at[0, slot]
            ),
            pltpu.make_async_copy(
                error_stage.at[slot], error_ref.at[:, k, :, pl.ds(s * LANES, LANES)], store_sem.at[1, slot]
            ),
        )

    for s in range(2):
        scales = [
            column_scale[:, s * half + c * LANES:s * half + (c + 1) * LANES] for c in range(OCT)
        ]

        def lattice(k, _, s=s, scales=scales):
            slot = lax.rem(k, 2)
            for peer in others:
                copy2(s, k, peer, peer).wait_recv()

            if s:
                for copy in stores(s, k, slot):
                    copy.wait()
            else:

                @pl.when(k >= 2)
                def _():
                    for copy in stores(s, k, slot):
                        copy.wait()

            def tile(j, _):
                at = pl.ds(pl.multiple_of(j * SUB, SUB), SUB)
                square = near = low = size = most = least = None
                for c in range(OCT):
                    q, part = c // slabs, c % slabs
                    rotated = in2[s, k, q, at, part * LANES:(part + 1) * LANES].astype(jnp.float32)
                    value = rotated * scales[c]
                    turned[at, c * LANES:(c + 1) * LANES] = value.astype(jnp.bfloat16)
                    nearest = jnp.round(value)
                    offset = jnp.abs(value - nearest)
                    below = jnp.floor(value)
                    if c == 0:
                        square, near, low, size = offset * offset, nearest, below, offset
                        most = least = offset
                    else:
                        square, near, low = square + offset * offset, near + nearest, low + below
                        size = size + offset
                        most, least = jnp.maximum(most, offset), jnp.minimum(least, offset)
                odd = near - 2.0 * jnp.floor(near * 0.5) > 0.5
                whole = jnp.where(odd, square + (1.0 - 2.0 * most), square)
                shifted = square + (OCT * 0.25 - size)
                odd = low - 2.0 * jnp.floor(low * 0.5) > 0.5
                error = jnp.minimum(whole, jnp.where(odd, shifted + 2.0 * least, shifted))
                error_stage[slot, j] = error
                row = me * (blocks * HB) + j * HB + k * SUB + lax.broadcasted_iota(jnp.int32, (SUB, LANES), 0)
                weight = (1.0 + 4.0 * (row.astype(jnp.float32) + 0.5) / total_rows) / 3.0
                sum_ref[...] += error * weight
                return 0

            lax.fori_loop(0, blocks, tile, 0)
            natural = jnp.dot(turned[...], p_ref[...], preferred_element_type=jnp.float32)
            scaled_stage[slot] = natural.astype(jnp.bfloat16).reshape(blocks, SUB, half)
            for copy in stores(s, k, slot):
                copy.start()
            return 0

        lax.fori_loop(0, FOLD, lattice, 0)

    for slot in range(2):
        for copy in stores(1, slot, slot):
            copy.wait()
    for s in range(2):
        for peer in others:
            copy1(s, peer, me).wait_send()
    for peer in others:
        copy3(peer, me).wait_send()

    def drain(k, _):
        for s in range(2):
            for peer in others:
                copy2(s, k, peer, me).wait_send()
        return 0

    lax.fori_loop(0, FOLD, drain, 0)


def body(weights, left_bits, right_bits, groups):
    _, local_rows, width = weights.shape
    peers = lax.axis_size("row")
    experts = lax.axis_size("expert")
    blocks = local_rows // HB
    half = width // 2
    lanes = half // peers
    rows = blocks * SUB
    scale = 1.0 / math.sqrt(width * HB)
    h = column_matrix(right_bits, peers, half, scale)
    left = (2 * left_bits - 1).astype(jnp.float32).reshape(blocks, HB, 1)
    ordered = groups.reshape(2, LANES, OCT).transpose(0, 2, 1).reshape(1, width)
    vmem = pl.BlockSpec(memory_space=pltpu.VMEM)
    hbm = pl.BlockSpec(memory_space=pl.ANY)
    dma = pltpu.SemaphoreType.DMA
    scaled, errors, group_scale, sums = pl.pallas_call(
        functools.partial(kernel, peers),
        out_shape=(
            jax.ShapeDtypeStruct((blocks, FOLD, SUB, width), jnp.bfloat16),
            jax.ShapeDtypeStruct((blocks, FOLD, SUB, width // OCT), jnp.float32),
            jax.ShapeDtypeStruct((8, LANES), jnp.float32),
            jax.ShapeDtypeStruct((SUB, LANES), jnp.float32),
        ),
        in_specs=[vmem] * 6,
        out_specs=(hbm, hbm, vmem, vmem),
        scratch_shapes=[
            pltpu.VMEM((2, peers, FOLD, rows, lanes), jnp.bfloat16),
            pltpu.VMEM((2, peers, FOLD, rows, lanes), jnp.bfloat16),
            pltpu.VMEM((2, FOLD, peers, rows, lanes), jnp.bfloat16),
            pltpu.VMEM((2, FOLD, peers, rows, lanes), jnp.bfloat16),
            pltpu.VMEM((peers, 2, 8, lanes), jnp.float32),
            pltpu.VMEM((rows, half), jnp.bfloat16),
            pltpu.VMEM((2, blocks, SUB, half), jnp.bfloat16),
            pltpu.VMEM((2, blocks, SUB, LANES), jnp.float32),
            dma((2, peers)),
            dma((2, peers)),
            dma((2, FOLD, peers)),
            dma((2, FOLD, peers)),
            dma((peers,)),
            dma((peers,)),
            dma((2, 2)),
        ],
        compiler_params=pltpu.CompilerParams(
            collective_id=0, has_side_effects=True, vmem_limit_bytes=60 * 2**20
        ),
    )(weights.reshape(blocks, HB, width), left, ordered, h, row_matrix(), order_matrix(half))
    partial_error = jnp.sum(sums) / (local_rows * peers * width // OCT)
    mine = lax.axis_index("expert")
    spread = jnp.where(jnp.arange(experts) == mine, partial_error, 0.0)
    every = lax.psum(spread, ("row", "expert"))
    expert_error = lax.dynamic_slice_in_dim(every, mine, 1)
    return (
        scaled.reshape(1, local_rows, width),
        errors.reshape(1, local_rows, width // OCT),
        group_scale[:1, :GROUPS],
        expert_error,
        jnp.sum(every) / experts,
    )


def solution(mesh):
    placed = (P("expert", "row", None), P("expert", "row"), P("expert", None), P("expert", None))
    return jax.shard_map(
        body,
        mesh=mesh,
        in_specs=placed,
        out_specs=(
            P("expert", "row", None),
            P("expert", "row", None),
            P("expert", None),
            P("expert"),
            P(),
        ),
        check_vma=False,
    )
```

```python
import functools
import math

import jax
import jax.numpy as jnp
from jax import lax
from jax.experimental import pallas as pl
from jax.experimental.pallas import tpu as pltpu
from jax.sharding import PartitionSpec as P

HB = 128
SUB = 16
FOLD = HB // SUB
OCT = 8
LANES = 128
GROUPS = 16
BLOCKS = 56
MESH = pl.DeviceIdType.MESH


def signs(common, bits):
    for shift in (4, 2, 1):
        if shift < bits:
            common = common ^ (common >> shift)
    return (1 - 2 * (common & 1)).astype(jnp.float32)


def iota(shape, dim):
    return lax.broadcasted_iota(jnp.int32, shape, dim)


def down(row):
    return jnp.broadcast_to(row, (LANES, LANES)).T


def cosine_block(order):
    first = jnp.arange(order, dtype=jnp.float32)[:, None]
    second = jnp.arange(order, dtype=jnp.float32)[None, :]
    table = math.sqrt(2.0 / order) * jnp.cos(math.pi * (2.0 * second + 1.0) * first / (2.0 * order))
    return jnp.where(first == 0.0, table * math.sqrt(0.5), table)


def build_column(right_ref, h_ref, scale):
    slabs = h_ref.shape[3] // LANES
    half = h_ref.shape[2]
    square = (LANES, LANES)
    octave = [signs((iota(square, 0) & (OCT - 1)) & s, 3) for s in range(OCT)]

    def step(u, _):
        at = pl.ds(pl.multiple_of(u * LANES, LANES), LANES)
        outer = signs(((u * LANES + iota(square, 0)) >> 3) & iota(square, 1), 7)
        for side in range(2):
            bits = right_ref[:, pl.ds(pl.multiple_of(side * half + u * LANES, LANES), LANES)]
            part = outer * down((2 * bits - 1).astype(jnp.float32) * scale)
            for s in range(OCT):
                q, slab = s // slabs, s % slabs
                h_ref[side, q, at, slab * LANES:(slab + 1) * LANES] = (part * octave[s]).astype(jnp.bfloat16)
        return 0

    lax.fori_loop(0, half // LANES, step, 0)


def build_left(left_ref, left):
    def step(j, _):
        bits = left_ref[:, pl.ds(pl.multiple_of(j * HB, HB), HB)]
        left[j] = down((2 * bits - 1).astype(jnp.float32))
        return 0

    lax.fori_loop(0, left.shape[0], step, 0)


def build_row(cosine_ref, m_ref):
    size = m_ref.shape[0]
    spread = (iota((size, BLOCKS), 0) // SUB == iota((size, BLOCKS), 1)).astype(jnp.float32).astype(jnp.bfloat16)
    chunk = size // 7

    def step(u, _):
        at = pl.multiple_of(u * chunk, chunk)
        here = ((at + iota((chunk, BLOCKS), 0)) // SUB == iota((chunk, BLOCKS), 1)).astype(jnp.float32)
        rows = jnp.dot(here.astype(jnp.bfloat16), cosine_ref[...], preferred_element_type=jnp.float32)
        full = lax.dot_general(
            rows.astype(jnp.bfloat16), spread, (((1,), (1,)), ((), ())), preferred_element_type=jnp.float32
        )
        small = signs((iota((chunk, size), 0) & iota((chunk, size), 1)) & (SUB - 1), 4)
        m_ref[pl.ds(at, chunk), :] = (full * small).astype(jnp.bfloat16)
        return 0

    lax.fori_loop(0, 7, step, 0)


def build_order(p_ref):
    half = p_ref.shape[0]

    def step(s, _):
        wanted = iota((LANES, half), 0) * OCT + s
        hit = (wanted == iota((LANES, half), 1)).astype(jnp.float32)
        p_ref[pl.ds(pl.multiple_of(s * LANES, LANES), LANES), :] = hit.astype(jnp.bfloat16)
        return 0

    lax.fori_loop(0, OCT, step, 0)


def fold_rows(parts):
    step = 1
    while step < len(parts):
        mixed = list(parts)
        for k in range(len(parts)):
            if not k & step:
                mixed[k] = parts[k] + parts[k + step]
                mixed[k + step] = parts[k] - parts[k + step]
        parts, step = mixed, 2 * step
    return parts


def kernel(
    peers, experts, x_hbm, left_ref, right_ref, group_ref, cosine_ref,
    scaled_ref, error_ref, scale_ref, mean_ref, total_ref,
    x_ref, left, h_ref, m_ref, p_ref, out1, in1, out2, in2, peaks, turned, scaled_stage, error_stage,
    sum_ref, row_sums, expert_sums,
    send1, recv1, send2, recv2, send3, recv3, send4, recv4, send5, recv5, store_sem, load_sem,
):
    blocks, _, width = x_ref.shape
    half = width // 2
    lanes = h_ref.shape[3]
    slabs = lanes // LANES
    rows = blocks * SUB
    me = lax.axis_index("row")
    mine = lax.axis_index("expert")
    load = pltpu.make_async_copy(x_hbm, x_ref, load_sem)
    load.start()
    far_first = sorted(range(1, peers), key=lambda d: (abs(d - peers // 2), d))
    others = [lax.rem(me + d, peers) for d in far_first]
    elsewhere = [lax.rem(mine + d, experts) for d in range(1, experts)]

    def remote(src, dst, send_sem, recv_sem, peer):
        return pltpu.make_async_remote_copy(
            src_ref=src, dst_ref=dst, send_sem=send_sem, recv_sem=recv_sem,
            device_id={"row": peer}, device_id_type=MESH,
        )

    def copy1(s, peer, land):
        return remote(out1.at[s, peer], in1.at[s, land], send1.at[s, peer], recv1.at[s, land], peer)

    def copy2(s, k, peer, land):
        return remote(
            out2.at[s, k, peer], in2.at[s, k, land], send2.at[s, k, peer], recv2.at[s, k, land], peer
        )

    def copy3(peer, land):
        return remote(peaks.at[me], peaks.at[land], send3.at[peer], recv3.at[land], peer)

    def copy4(peer, land):
        return remote(row_sums.at[me], row_sums.at[land], send4.at[peer], recv4.at[land], peer)

    def copy5(peer, land):
        return pltpu.make_async_remote_copy(
            src_ref=expert_sums.at[mine], dst_ref=expert_sums.at[land],
            send_sem=send5.at[peer], recv_sem=recv5.at[land],
            device_id={"expert": peer}, device_id_type=MESH,
        )

    barrier = pltpu.get_barrier_semaphore()
    for peer in others:
        pl.semaphore_signal(barrier, inc=1, device_id={"row": peer}, device_id_type=MESH)
    for peer in elsewhere:
        pl.semaphore_signal(barrier, inc=1, device_id={"expert": peer}, device_id_type=MESH)
    build_column(right_ref, h_ref, 1.0 / math.sqrt(width * HB))
    build_left(left_ref, left)
    load.wait()

    def column_side(peer, dst, place):
        def step(j, _):
            low = jnp.dot(x_ref[j, :, :half], h_ref[0, peer], preferred_element_type=jnp.float32)
            high = jnp.dot(x_ref[j, :, half:], h_ref[1, peer], preferred_element_type=jnp.float32)
            sign = jnp.concatenate([left[j]] * slabs, axis=1)
            for s, both in ((0, low + high), (1, low - high)):
                both = both * sign
                parts = fold_rows([both[k * SUB:(k + 1) * SUB] for k in range(FOLD)])
                for k in range(FOLD):
                    dst[s, place, k, pl.ds(pl.multiple_of(j * SUB, SUB), SUB), :] = parts[k].astype(jnp.bfloat16)
            return 0

        lax.fori_loop(0, blocks, step, 0)

    for step, peer in enumerate(others):
        column_side(peer, out1, peer)
        if step == 0:
            pl.semaphore_wait(barrier, peers + experts - 2)
        copy1(0, peer, me).start()
    for peer in others:
        copy1(1, peer, me).start()
    column_side(me, in1, me)
    build_row(cosine_ref, m_ref)
    build_order(p_ref)

    def row_side(s, send):
        for peer in others:
            copy1(s, peer, peer).wait_recv()

        def step(k, peak):
            z = in1[s, :, k].reshape(peers * rows, lanes)
            r = jnp.dot(m_ref[...], z, preferred_element_type=jnp.float32)
            out2[s, k] = r.astype(jnp.bfloat16).reshape(peers, rows, lanes)
            if send:
                for peer in others:
                    copy2(s, k, peer, me).start()
            return jnp.maximum(peak, jnp.max(jnp.abs(r).reshape(-1, 8, lanes), axis=0))

        peak = lax.fori_loop(0, FOLD, step, jnp.zeros((8, lanes), jnp.float32))
        peaks[me, s] = jnp.broadcast_to(jnp.max(peak, axis=0, keepdims=True), (8, lanes))

    row_side(0, True)
    row_side(1, False)
    for peer in others:
        copy3(peer, me).start()

    def send_second(k, _):
        for peer in others:
            copy2(1, k, peer, me).start()
        return 0

    lax.fori_loop(0, FOLD, send_second, 0)

    def keep_own(k, _):
        for s in range(2):
            in2[s, k, me] = out2[s, k, me]
        return 0

    lax.fori_loop(0, FOLD, keep_own, 0)

    for peer in others:
        copy3(peer, peer).wait_recv()
    column_peak = jnp.concatenate([peaks[q, s, 0:1, :] for s in range(2) for q in range(peers)], axis=1)
    spread = jnp.broadcast_to(group_ref[...], (8, width)).astype(jnp.float32).astype(jnp.bfloat16)
    group = jnp.concatenate([
        lax.dot_general(
            spread[:, s * half:(s + 1) * half], p_ref[...], (((1,), (1,)), ((), ())),
            preferred_element_type=jnp.float32,
        )[:1]
        for s in range(2)
    ], axis=1)
    column_scale = jnp.zeros_like(column_peak)
    group_scale = jnp.zeros((8, LANES), jnp.float32)
    lane = lax.broadcasted_iota(jnp.int32, (8, LANES), 1)
    for g in range(GROUPS):
        inside = group == float(g)
        peak = jnp.maximum(jnp.max(jnp.where(inside, column_peak, 0.0), axis=1, keepdims=True), 1.0)
        column_scale = jnp.where(inside, 2.0 / peak, column_scale)
        group_scale = jnp.where(lane == g, peak * 0.5, group_scale)
    scale_ref[...] = group_scale[:1, :GROUPS]
    sum_ref[...] = jnp.zeros_like(sum_ref)

    total_rows = peers * blocks * HB

    def stores(s, k, slot):
        return (
            pltpu.make_async_copy(
                scaled_stage.at[slot], scaled_ref.at[:, k, :, pl.ds(s * half, half)], store_sem.at[0, slot]
            ),
            pltpu.make_async_copy(
                error_stage.at[slot], error_ref.at[:, k, :, pl.ds(s * LANES, LANES)], store_sem.at[1, slot]
            ),
        )

    for s in range(2):
        scales = [
            column_scale[:, s * half + c * LANES:s * half + (c + 1) * LANES] for c in range(OCT)
        ]

        def lattice(k, _, s=s, scales=scales):
            slot = lax.rem(k, 2)
            for peer in others:
                copy2(s, k, peer, peer).wait_recv()

            if s:
                for copy in stores(s, k, slot):
                    copy.wait()
            else:

                @pl.when(k >= 2)
                def _():
                    for copy in stores(s, k, slot):
                        copy.wait()

            def tile(j, _):
                at = pl.ds(pl.multiple_of(j * SUB, SUB), SUB)
                square = near = low = size = most = least = None
                for c in range(OCT):
                    q, part = c // slabs, c % slabs
                    rotated = in2[s, k, q, at, part * LANES:(part + 1) * LANES].astype(jnp.float32)
                    value = rotated * scales[c]
                    turned[at, c * LANES:(c + 1) * LANES] = value.astype(jnp.bfloat16)
                    nearest = jnp.round(value)
                    offset = jnp.abs(value - nearest)
                    below = jnp.floor(value)
                    if c == 0:
                        square, near, low, size = offset * offset, nearest, below, offset
                        most = least = offset
                    else:
                        square, near, low = square + offset * offset, near + nearest, low + below
                        size = size + offset
                        most, least = jnp.maximum(most, offset), jnp.minimum(least, offset)
                odd = near - 2.0 * jnp.floor(near * 0.5) > 0.5
                whole = jnp.where(odd, square + (1.0 - 2.0 * most), square)
                shifted = square + (OCT * 0.25 - size)
                odd = low - 2.0 * jnp.floor(low * 0.5) > 0.5
                error = jnp.minimum(whole, jnp.where(odd, shifted + 2.0 * least, shifted))
                error_stage[slot, j] = error
                row = me * (blocks * HB) + j * HB + k * SUB + lax.broadcasted_iota(jnp.int32, (SUB, LANES), 0)
                weight = (1.0 + 4.0 * (row.astype(jnp.float32) + 0.5) / total_rows) / 3.0
                sum_ref[...] += error * weight
                return 0

            lax.fori_loop(0, blocks, tile, 0)
            natural = jnp.dot(turned[...], p_ref[...], preferred_element_type=jnp.float32)
            scaled_stage[slot] = natural.astype(jnp.bfloat16).reshape(blocks, SUB, half)
            for copy in stores(s, k, slot):
                copy.start()
            return 0

        lax.fori_loop(0, FOLD, lattice, 0)

    part = jnp.sum(jnp.sum(sum_ref[...], axis=0, keepdims=True), axis=1, keepdims=True)
    row_sums[me] = jnp.broadcast_to(part / (total_rows * width // OCT), (8, LANES))
    for peer in others:
        copy4(peer, me).start()
    for peer in others:
        copy4(peer, peer).wait_recv()
    mean = row_sums[0]
    for q in range(1, peers):
        mean = mean + row_sums[q]
    expert_sums[mine] = mean
    for peer in elsewhere:
        copy5(peer, mine).start()
    for peer in elsewhere:
        copy5(peer, peer).wait_recv()
    total = expert_sums[0]
    for e in range(1, experts):
        total = total + expert_sums[e]
    mean_ref[0] = jnp.max(mean)
    total_ref[0] = jnp.max(total / experts)

    for slot in range(2):
        for copy in stores(1, slot, slot):
            copy.wait()
    for s in range(2):
        for peer in others:
            copy1(s, peer, me).wait_send()
    for peer in others:
        copy3(peer, me).wait_send()
        copy4(peer, me).wait_send()
    for peer in elsewhere:
        copy5(peer, mine).wait_send()

    def drain(k, _):
        for s in range(2):
            for peer in others:
                copy2(s, k, peer, me).wait_send()
        return 0

    lax.fori_loop(0, FOLD, drain, 0)


def body(weights, left_bits, right_bits, groups):
    _, local_rows, width = weights.shape
    peers = lax.axis_size("row")
    experts = lax.axis_size("expert")
    blocks = local_rows // HB
    half = width // 2
    lanes = half // peers
    rows = blocks * SUB
    cosine = cosine_block(BLOCKS).astype(jnp.bfloat16)
    vmem = pl.BlockSpec(memory_space=pltpu.VMEM)
    hbm = pl.BlockSpec(memory_space=pl.ANY)
    dma = pltpu.SemaphoreType.DMA
    smem = pl.BlockSpec(memory_space=pltpu.SMEM)
    scaled, errors, group_scale, mean, total = pl.pallas_call(
        functools.partial(kernel, peers, experts),
        out_shape=(
            jax.ShapeDtypeStruct((blocks, FOLD, SUB, width), jnp.bfloat16),
            jax.ShapeDtypeStruct((blocks, FOLD, SUB, width // OCT), jnp.float32),
            jax.ShapeDtypeStruct((1, GROUPS), jnp.float32),
            jax.ShapeDtypeStruct((1,), jnp.float32),
            jax.ShapeDtypeStruct((1,), jnp.float32),
        ),
        in_specs=[hbm] + [vmem] * 4,
        out_specs=(hbm, hbm, vmem, smem, smem),
        scratch_shapes=[
            pltpu.VMEM((blocks, HB, width), jnp.bfloat16),
            pltpu.VMEM((blocks, HB, LANES), jnp.float32),
            pltpu.VMEM((2, peers, half, lanes), jnp.bfloat16),
            pltpu.VMEM((BLOCKS * SUB, BLOCKS * SUB), jnp.bfloat16),
            pltpu.VMEM((half, half), jnp.bfloat16),
            pltpu.VMEM((2, peers, FOLD, rows, lanes), jnp.bfloat16),
            pltpu.VMEM((2, peers, FOLD, rows, lanes), jnp.bfloat16),
            pltpu.VMEM((2, FOLD, peers, rows, lanes), jnp.bfloat16),
            pltpu.VMEM((2, FOLD, peers, rows, lanes), jnp.bfloat16),
            pltpu.VMEM((peers, 2, 8, lanes), jnp.float32),
            pltpu.VMEM((rows, half), jnp.bfloat16),
            pltpu.VMEM((2, blocks, SUB, half), jnp.bfloat16),
            pltpu.VMEM((2, blocks, SUB, LANES), jnp.float32),
            pltpu.VMEM((SUB, LANES), jnp.float32),
            pltpu.VMEM((peers, 8, LANES), jnp.float32),
            pltpu.VMEM((experts, 8, LANES), jnp.float32),
            dma((2, peers)),
            dma((2, peers)),
            dma((2, FOLD, peers)),
            dma((2, FOLD, peers)),
            dma((peers,)),
            dma((peers,)),
            dma((peers,)),
            dma((peers,)),
            dma((experts,)),
            dma((experts,)),
            dma((2, 2)),
            dma,
        ],
        compiler_params=pltpu.CompilerParams(
            collective_id=0, has_side_effects=True, vmem_limit_bytes=60 * 2**20
        ),
    )(weights.reshape(blocks, HB, width), left_bits, right_bits, groups, cosine)
    return (
        scaled.reshape(1, local_rows, width),
        errors.reshape(1, local_rows, width // OCT),
        group_scale,
        mean,
        total.reshape(()),
    )


def solution(mesh):
    placed = (P("expert", "row", None), P("expert", "row"), P("expert", None), P("expert", None))
    return jax.shard_map(
        body,
        mesh=mesh,
        in_specs=placed,
        out_specs=(
            P("expert", "row", None),
            P("expert", "row", None),
            P("expert", None),
            P("expert"),
            P(),
        ),
        check_vma=False,
    )
```

```python
import functools
import math

import jax
import jax.numpy as jnp
from jax import lax
from jax.experimental import pallas as pl
from jax.experimental.pallas import tpu as pltpu
from jax.sharding import PartitionSpec as P

HB = 128
SUB = 16
FOLD = HB // SUB
OCT = 8
LANES = 128
GROUPS = 16
BLOCKS = 56
MESH = pl.DeviceIdType.MESH


def signs(common, bits):
    for shift in (4, 2, 1):
        if shift < bits:
            common = common ^ (common >> shift)
    return (1 - 2 * (common & 1)).astype(jnp.float32)


def iota(shape, dim):
    return lax.broadcasted_iota(jnp.int32, shape, dim)


def down(row):
    return jnp.broadcast_to(row, (LANES, LANES)).T


def cosine_block(order):
    first = jnp.arange(order, dtype=jnp.float32)[:, None]
    second = jnp.arange(order, dtype=jnp.float32)[None, :]
    table = math.sqrt(2.0 / order) * jnp.cos(math.pi * (2.0 * second + 1.0) * first / (2.0 * order))
    return jnp.where(first == 0.0, table * math.sqrt(0.5), table)


def build_column(right_ref, h_ref, scale):
    slabs = h_ref.shape[3] // LANES
    half = h_ref.shape[2]
    square = (LANES, LANES)
    octave = [signs((iota(square, 0) & (OCT - 1)) & s, 3) for s in range(OCT)]

    def step(u, _):
        at = pl.ds(pl.multiple_of(u * LANES, LANES), LANES)
        outer = signs(((u * LANES + iota(square, 0)) >> 3) & iota(square, 1), 7)
        for side in range(2):
            bits = right_ref[:, pl.ds(pl.multiple_of(side * half + u * LANES, LANES), LANES)]
            part = outer * down((2 * bits - 1).astype(jnp.float32) * scale)
            for s in range(OCT):
                q, slab = s // slabs, s % slabs
                h_ref[side, q, at, slab * LANES:(slab + 1) * LANES] = (part * octave[s]).astype(jnp.bfloat16)
        return 0

    lax.fori_loop(0, half // LANES, step, 0)


def build_left(left_ref, left):
    def step(j, _):
        bits = left_ref[:, pl.ds(pl.multiple_of(j * HB, HB), HB)]
        left[j] = down((2 * bits - 1).astype(jnp.float32))
        return 0

    lax.fori_loop(0, left.shape[0], step, 0)


def build_row(cosine_ref, m_ref):
    size = m_ref.shape[0]
    spread = (iota((size, BLOCKS), 0) // SUB == iota((size, BLOCKS), 1)).astype(jnp.float32).astype(jnp.bfloat16)
    chunk = size // 7

    def step(u, _):
        at = pl.multiple_of(u * chunk, chunk)
        here = ((at + iota((chunk, BLOCKS), 0)) // SUB == iota((chunk, BLOCKS), 1)).astype(jnp.float32)
        rows = jnp.dot(here.astype(jnp.bfloat16), cosine_ref[...], preferred_element_type=jnp.float32)
        full = lax.dot_general(
            rows.astype(jnp.bfloat16), spread, (((1,), (1,)), ((), ())), preferred_element_type=jnp.float32
        )
        small = signs((iota((chunk, size), 0) & iota((chunk, size), 1)) & (SUB - 1), 4)
        m_ref[pl.ds(at, chunk), :] = (full * small).astype(jnp.bfloat16)
        return 0

    lax.fori_loop(0, 7, step, 0)


def build_order(p_ref):
    half = p_ref.shape[0]

    def step(s, _):
        wanted = iota((LANES, half), 0) * OCT + s
        hit = (wanted == iota((LANES, half), 1)).astype(jnp.float32)
        p_ref[pl.ds(pl.multiple_of(s * LANES, LANES), LANES), :] = hit.astype(jnp.bfloat16)
        return 0

    lax.fori_loop(0, OCT, step, 0)


def fold_rows(parts):
    step = 1
    while step < len(parts):
        mixed = list(parts)
        for k in range(len(parts)):
            if not k & step:
                mixed[k] = parts[k] + parts[k + step]
                mixed[k + step] = parts[k] - parts[k + step]
        parts, step = mixed, 2 * step
    return parts


def kernel(
    peers, experts, x_hbm, left_ref, right_ref, group_ref, cosine_ref,
    scaled_ref, error_ref, scale_ref, mean_ref, total_ref,
    x_ref, left, h_ref, m_ref, p_ref, out1, in1, out2, in2, peaks, turned,
    sum_ref, row_sums, expert_sums,
    send1, recv1, send2, recv2, send3, recv3, send4, recv4, send5, recv5, load_sem,
):
    blocks, _, width = x_ref.shape
    half = width // 2
    lanes = h_ref.shape[3]
    slabs = lanes // LANES
    rows = blocks * SUB
    me = lax.axis_index("row")
    mine = lax.axis_index("expert")
    load = pltpu.make_async_copy(x_hbm, x_ref, load_sem)
    load.start()
    far_first = sorted(range(1, peers), key=lambda d: (abs(d - peers // 2), d))
    others = [lax.rem(me + d, peers) for d in far_first]
    elsewhere = [lax.rem(mine + d, experts) for d in range(1, experts)]

    def remote(src, dst, send_sem, recv_sem, peer):
        return pltpu.make_async_remote_copy(
            src_ref=src, dst_ref=dst, send_sem=send_sem, recv_sem=recv_sem,
            device_id={"row": peer}, device_id_type=MESH,
        )

    def copy1(s, peer, land):
        return remote(out1.at[s, peer], in1.at[s, land], send1.at[s, peer], recv1.at[s, land], peer)

    def copy2(s, k, peer, land):
        return remote(
            out2.at[s, k, peer], in2.at[s, k, land], send2.at[s, k, peer], recv2.at[s, k, land], peer
        )

    def copy3(peer, land):
        return remote(peaks.at[me], peaks.at[land], send3.at[peer], recv3.at[land], peer)

    def copy4(peer, land):
        return remote(row_sums.at[me], row_sums.at[land], send4.at[peer], recv4.at[land], peer)

    def copy5(peer, land):
        return pltpu.make_async_remote_copy(
            src_ref=expert_sums.at[mine], dst_ref=expert_sums.at[land],
            send_sem=send5.at[peer], recv_sem=recv5.at[land],
            device_id={"expert": peer}, device_id_type=MESH,
        )

    barrier = pltpu.get_barrier_semaphore()
    for peer in others:
        pl.semaphore_signal(barrier, inc=1, device_id={"row": peer}, device_id_type=MESH)
    for peer in elsewhere:
        pl.semaphore_signal(barrier, inc=1, device_id={"expert": peer}, device_id_type=MESH)
    build_column(right_ref, h_ref, 1.0 / math.sqrt(width * HB))
    build_left(left_ref, left)
    load.wait()

    def column_side(peer, dst, place):
        def step(j, _):
            low = jnp.dot(x_ref[j, :, :half], h_ref[0, peer], preferred_element_type=jnp.float32)
            high = jnp.dot(x_ref[j, :, half:], h_ref[1, peer], preferred_element_type=jnp.float32)
            sign = jnp.concatenate([left[j]] * slabs, axis=1)
            for s, both in ((0, low + high), (1, low - high)):
                both = both * sign
                parts = fold_rows([both[k * SUB:(k + 1) * SUB] for k in range(FOLD)])
                for k in range(FOLD):
                    dst[s, place, k, pl.ds(pl.multiple_of(j * SUB, SUB), SUB), :] = parts[k].astype(jnp.bfloat16)
            return 0

        lax.fori_loop(0, blocks, step, 0)

    for step, peer in enumerate(others):
        column_side(peer, out1, peer)
        if step == 0:
            pl.semaphore_wait(barrier, peers + experts - 2)
        copy1(0, peer, me).start()
    for peer in others:
        copy1(1, peer, me).start()
    column_side(me, in1, me)
    build_row(cosine_ref, m_ref)
    build_order(p_ref)

    def row_side(s, send):
        for peer in others:
            copy1(s, peer, peer).wait_recv()

        def step(k, peak):
            z = in1[s, :, k].reshape(peers * rows, lanes)
            r = jnp.dot(m_ref[...], z, preferred_element_type=jnp.float32)
            out2[s, k] = r.astype(jnp.bfloat16).reshape(peers, rows, lanes)
            if send:
                for peer in others:
                    copy2(s, k, peer, me).start()
            return jnp.maximum(peak, jnp.max(jnp.abs(r).reshape(-1, 8, lanes), axis=0))

        peak = lax.fori_loop(0, FOLD, step, jnp.zeros((8, lanes), jnp.float32))
        peaks[me, s] = jnp.broadcast_to(jnp.max(peak, axis=0, keepdims=True), (8, lanes))

    row_side(0, True)
    row_side(1, False)
    for peer in others:
        copy3(peer, me).start()

    def send_second(k, _):
        for peer in others:
            copy2(1, k, peer, me).start()
        return 0

    lax.fori_loop(0, FOLD, send_second, 0)

    def keep_own(k, _):
        for s in range(2):
            in2[s, k, me] = out2[s, k, me]
        return 0

    lax.fori_loop(0, FOLD, keep_own, 0)

    for peer in others:
        copy3(peer, peer).wait_recv()
    column_peak = jnp.concatenate([peaks[q, s, 0:1, :] for s in range(2) for q in range(peers)], axis=1)
    spread = jnp.broadcast_to(group_ref[...], (8, width)).astype(jnp.float32).astype(jnp.bfloat16)
    group = jnp.concatenate([
        lax.dot_general(
            spread[:, s * half:(s + 1) * half], p_ref[...], (((1,), (1,)), ((), ())),
            preferred_element_type=jnp.float32,
        )[:1]
        for s in range(2)
    ], axis=1)
    column_scale = jnp.zeros_like(column_peak)
    group_scale = jnp.zeros((8, LANES), jnp.float32)
    lane = lax.broadcasted_iota(jnp.int32, (8, LANES), 1)
    for g in range(GROUPS):
        inside = group == float(g)
        peak = jnp.maximum(jnp.max(jnp.where(inside, column_peak, 0.0), axis=1, keepdims=True), 1.0)
        column_scale = jnp.where(inside, 2.0 / peak, column_scale)
        group_scale = jnp.where(lane == g, peak * 0.5, group_scale)
    scale_ref[...] = group_scale[:1, :GROUPS]
    sum_ref[...] = jnp.zeros_like(sum_ref)

    total_rows = peers * blocks * HB

    for s in range(2):
        scales = [
            column_scale[:, s * half + c * LANES:s * half + (c + 1) * LANES] for c in range(OCT)
        ]

        def lattice(k, _, s=s, scales=scales):
            for peer in others:
                copy2(s, k, peer, peer).wait_recv()

            def tile(j, _):
                at = pl.ds(pl.multiple_of(j * SUB, SUB), SUB)
                square = near = low = size = most = least = None
                for c in range(OCT):
                    q, part = c // slabs, c % slabs
                    rotated = in2[s, k, q, at, part * LANES:(part + 1) * LANES].astype(jnp.float32)
                    value = rotated * scales[c]
                    turned[at, c * LANES:(c + 1) * LANES] = value.astype(jnp.bfloat16)
                    nearest = jnp.round(value)
                    offset = jnp.abs(value - nearest)
                    below = jnp.floor(value)
                    if c == 0:
                        square, near, low, size = offset * offset, nearest, below, offset
                        most = least = offset
                    else:
                        square, near, low = square + offset * offset, near + nearest, low + below
                        size = size + offset
                        most, least = jnp.maximum(most, offset), jnp.minimum(least, offset)
                odd = near - 2.0 * jnp.floor(near * 0.5) > 0.5
                whole = jnp.where(odd, square + (1.0 - 2.0 * most), square)
                shifted = square + (OCT * 0.25 - size)
                odd = low - 2.0 * jnp.floor(low * 0.5) > 0.5
                error = jnp.minimum(whole, jnp.where(odd, shifted + 2.0 * least, shifted))
                error_ref[j, k, :, s * LANES:(s + 1) * LANES] = error
                row = me * (blocks * HB) + j * HB + k * SUB + lax.broadcasted_iota(jnp.int32, (SUB, LANES), 0)
                weight = (1.0 + 4.0 * (row.astype(jnp.float32) + 0.5) / total_rows) / 3.0
                sum_ref[...] += error * weight
                return 0

            lax.fori_loop(0, blocks, tile, 0)
            natural = jnp.dot(turned[...], p_ref[...], preferred_element_type=jnp.float32)
            scaled_ref[:, k, :, s * half:(s + 1) * half] = natural.astype(jnp.bfloat16).reshape(blocks, SUB, half)
            return 0

        lax.fori_loop(0, FOLD, lattice, 0)

    part = jnp.sum(jnp.sum(sum_ref[...], axis=0, keepdims=True), axis=1, keepdims=True)
    row_sums[me] = jnp.broadcast_to(part / (total_rows * width // OCT), (8, LANES))
    for peer in others:
        copy4(peer, me).start()
    for peer in others:
        copy4(peer, peer).wait_recv()
    mean = row_sums[0]
    for q in range(1, peers):
        mean = mean + row_sums[q]
    expert_sums[mine] = mean
    for peer in elsewhere:
        copy5(peer, mine).start()
    for peer in elsewhere:
        copy5(peer, peer).wait_recv()
    total = expert_sums[0]
    for e in range(1, experts):
        total = total + expert_sums[e]
    mean_ref[0] = jnp.max(mean)
    total_ref[0] = jnp.max(total / experts)

    for s in range(2):
        for peer in others:
            copy1(s, peer, me).wait_send()
    for peer in others:
        copy3(peer, me).wait_send()
        copy4(peer, me).wait_send()
    for peer in elsewhere:
        copy5(peer, mine).wait_send()

    def drain(k, _):
        for s in range(2):
            for peer in others:
                copy2(s, k, peer, me).wait_send()
        return 0

    lax.fori_loop(0, FOLD, drain, 0)


def put_kernel(scaled_ref, error_ref, scaled_out, error_out, sems):
    copies = (
        pltpu.make_async_copy(scaled_ref, scaled_out, sems.at[0]),
        pltpu.make_async_copy(error_ref, error_out, sems.at[1]),
    )
    for copy in copies:
        copy.start()
    for copy in copies:
        copy.wait()


def put(scaled, errors):
    return pl.pallas_call(
        put_kernel,
        out_shape=(
            jax.ShapeDtypeStruct(scaled.shape, scaled.dtype),
            jax.ShapeDtypeStruct(errors.shape, errors.dtype),
        ),
        in_specs=[pl.BlockSpec(memory_space=pltpu.VMEM)] * 2,
        out_specs=[pl.BlockSpec(memory_space=pl.ANY)] * 2,
        scratch_shapes=[pltpu.SemaphoreType.DMA((2,))],
        compiler_params=pltpu.CompilerParams(vmem_limit_bytes=16 * 2**20),
    )(scaled, errors)


def body(weights, left_bits, right_bits, groups):
    _, local_rows, width = weights.shape
    peers = lax.axis_size("row")
    experts = lax.axis_size("expert")
    blocks = local_rows // HB
    half = width // 2
    lanes = half // peers
    rows = blocks * SUB
    cosine = cosine_block(BLOCKS).astype(jnp.bfloat16)
    vmem = pl.BlockSpec(memory_space=pltpu.VMEM)
    hbm = pl.BlockSpec(memory_space=pl.ANY)
    dma = pltpu.SemaphoreType.DMA
    smem = pl.BlockSpec(memory_space=pltpu.SMEM)
    scaled, errors, group_scale, mean, total = pl.pallas_call(
        functools.partial(kernel, peers, experts),
        out_shape=(
            pltpu.VMEM((blocks, FOLD, SUB, width), jnp.bfloat16),
            pltpu.VMEM((blocks, FOLD, SUB, width // OCT), jnp.float32),
            jax.ShapeDtypeStruct((1, GROUPS), jnp.float32),
            jax.ShapeDtypeStruct((1,), jnp.float32),
            jax.ShapeDtypeStruct((1,), jnp.float32),
        ),
        in_specs=[hbm] + [vmem] * 4,
        out_specs=(vmem, vmem, vmem, smem, smem),
        scratch_shapes=[
            pltpu.VMEM((blocks, HB, width), jnp.bfloat16),
            pltpu.VMEM((blocks, HB, LANES), jnp.float32),
            pltpu.VMEM((2, peers, half, lanes), jnp.bfloat16),
            pltpu.VMEM((BLOCKS * SUB, BLOCKS * SUB), jnp.bfloat16),
            pltpu.VMEM((half, half), jnp.bfloat16),
            pltpu.VMEM((2, peers, FOLD, rows, lanes), jnp.bfloat16),
            pltpu.VMEM((2, peers, FOLD, rows, lanes), jnp.bfloat16),
            pltpu.VMEM((2, FOLD, peers, rows, lanes), jnp.bfloat16),
            pltpu.VMEM((2, FOLD, peers, rows, lanes), jnp.bfloat16),
            pltpu.VMEM((peers, 2, 8, lanes), jnp.float32),
            pltpu.VMEM((rows, half), jnp.bfloat16),
            pltpu.VMEM((SUB, LANES), jnp.float32),
            pltpu.VMEM((peers, 8, LANES), jnp.float32),
            pltpu.VMEM((experts, 8, LANES), jnp.float32),
            dma((2, peers)),
            dma((2, peers)),
            dma((2, FOLD, peers)),
            dma((2, FOLD, peers)),
            dma((peers,)),
            dma((peers,)),
            dma((peers,)),
            dma((peers,)),
            dma((experts,)),
            dma((experts,)),
            dma,
        ],
        compiler_params=pltpu.CompilerParams(
            collective_id=0, has_side_effects=True, vmem_limit_bytes=48 * 2**20
        ),
    )(weights.reshape(blocks, HB, width), left_bits, right_bits, groups, cosine)
    scaled, errors = put(scaled, errors)
    return (
        scaled.reshape(1, local_rows, width),
        errors.reshape(1, local_rows, width // OCT),
        group_scale,
        mean,
        total.reshape(()),
    )


def solution(mesh):
    placed = (P("expert", "row", None), P("expert", "row"), P("expert", None), P("expert", None))
    return jax.shard_map(
        body,
        mesh=mesh,
        in_specs=placed,
        out_specs=(
            P("expert", "row", None),
            P("expert", "row", None),
            P("expert", None),
            P("expert"),
            P(),
        ),
        check_vma=False,
    )
```
